32 devices in a mesh: pts: 8 (over y, x, core), cam: 4 (over z).
Axes of the slice: x: 2, y: 2, z: 4, core: 2. Of those that a mesh axis runs over, the one named last changes fastest.
Arguments:
- cameras: float32 [9, 4096], P(None, ('pts', 'cam')), may hold values from -0.5 to 2
- increment: float32 [9, 4096], P(None, ('pts', 'cam')), may hold values from -0.3 to 0.3
- points: float32 [3, 524288], P(None, 'pts'), may hold values from -6 to 2
- point_gradient: float32 [3, 524288], P(None, 'pts'), may hold values from -1.8 to 1.8
- point_inverse: float32 [9, 524288], P(None, 'pts'), may hold values from -0.35 to 1.6, as said below
- cam_jacobian: bfloat16 [18, 8388608], P(None, ('pts', 'cam')), may hold values from -3 to 3
- point_jacobian: bfloat16 [6, 8388608], P(None, ('pts', 'cam')), may hold values from -3 to 3
- observed: float32 [2, 8388608], P(None, ('pts', 'cam')), may hold values from -10 to 10
- tile_block: int32 [32768], P(('pts', 'cam')), may hold values from 0 to 31
- tile_points: int32 [32768], P(('pts', 'cam')), may hold values from 0 to 255
- obs_camera: int32 [8388608], P(('pts', 'cam')), may hold values from 0 to 127
- obs_point: int32 [8388608], P(('pts', 'cam')), may hold values from 0 to 255
- accept: int32 [], replicated, may hold values from 0 to 1073741823
Outputs:
- residual: float32 [2, 8388608], P(None, ('pts', 'cam'))
- trial_cost: float32 [], replicated
- accepted_points: float32 [3, 524288], P(None, 'pts')
- accepted_cameras: float32 [9, 4096], P(None, ('pts', 'cam'))
The draws below stay inside these ranges and needn't reach their ends.
Inputs may be any that keep to these rules, and one draw needn't show every extreme that they name: `tile_block`: the block of 128 cameras that all 256 observations of a tile look at. `tile_points`: the block of 256 points of its point group that all 256 observations of a tile look at. `obs_camera`: an observation's camera within its tile's block. `obs_point`: an observation's point within its tile's point block. `accept`: an odd word accepts the step, an even one keeps the old parameters. `point_inverse`: each 3 x 3 block is symmetric with a dominant positive diagonal.
All inputs are finite; a program needn't handle non-finite values.
Results may differ from the reference program's by a relative error of at most 0.0003.
Values sent between devices are 32-bit elements; how exact they have to be, the bound alone decides.
No kernel may reach another device: no remote copies, remote signals or barrier semaphores. Data moves between devices by JAX's collectives and lax.ppermute only.
A program may use at most 192 MiB of HBM per device.

```python
import math
import jax
import jax.numpy as jnp
from jax import lax

CB = 128
PB = 256
TILE = 256
PTS_DEV = 65536
OBS_GROUP = 1048576
NOBS = 8388608
NPTS = 524288
CAMS = 4096
N_PTS = 8


def draw_cameras(key, part):
    keys = jax.random.split(jax.random.fold_in(key, 11), 4)
    rotation = jax.random.uniform(keys[0], (3, CAMS), jnp.float32, -0.3, 0.3)
    shifted = jnp.clip(0.2 * jax.random.normal(keys[1], (3, CAMS), jnp.float32), -0.5, 0.5)
    focal = jax.random.uniform(keys[2], (1, CAMS), jnp.float32, 0.6, 1.4)
    radial = jax.random.uniform(keys[3], (2, CAMS), jnp.float32, -1.0, 1.0) * jnp.array([[0.05], [0.005]], jnp.float32)
    return jnp.concatenate([rotation, shifted, focal, radial], axis=0)


def draw_increment(key, part):
    keys = jax.random.split(jax.random.fold_in(key, 17), 1)
    scales = jnp.array([0.05, 0.05, 0.05, 0.1, 0.1, 0.1, 0.05, 0.01, 0.002], jnp.float32).reshape(9, 1)
    values = jnp.clip(jax.random.normal(keys[0], (9, CAMS), jnp.float32), -3.0, 3.0)
    return values * scales


def draw_points(key, part):
    keys = jax.random.split(jax.random.fold_in(key, 19), 2)
    planar = jax.random.uniform(keys[0], (2, NPTS), jnp.float32, -2.0, 2.0)
    height = jax.random.uniform(keys[1], (1, NPTS), jnp.float32, -6.0, -0.8)
    return jnp.concatenate([planar, height], axis=0)


def draw_point_inverse(key, part):
    keys = jax.random.split(jax.random.fold_in(key, 23), 2)
    diagonal = jax.random.uniform(keys[0], (3, NPTS), jnp.float32, 0.8, 1.6)
    offdiag = jax.random.uniform(keys[1], (3, NPTS), jnp.float32, -0.35, 0.35)
    return jnp.stack([diagonal[0], offdiag[0], offdiag[1], offdiag[0], diagonal[1], offdiag[2], offdiag[1], offdiag[2], diagonal[2]])


def draw_observed(key, part):
    keys = jax.random.split(jax.random.fold_in(key, 29), 2)
    position = lax_free_iota()
    level = 0.5 * jnp.exp(math.log(3.0) * position / NOBS)
    spread = jnp.exp(jax.random.uniform(keys[1], (2, NOBS), jnp.float32, math.log(0.5), math.log(2.0)))
    values = jnp.clip(jax.random.normal(keys[0], (2, NOBS), jnp.float32), -3.0, 3.0)
    return values * level * spread


def lax_free_iota():
    return jnp.arange(NOBS, dtype=jnp.float32).reshape(1, NOBS)


def plant(entries, key, smallest, high):
    shape = entries.shape
    place = [jax.random.randint(jax.random.fold_in(key, axis), (), 0, shape[axis]) for axis in range(len(shape))]
    entries = entries.at[tuple(place)].set(smallest)
    longest = shape.index(max(shape))
    place[longest] = (place[longest] + 1) % shape[longest]
    return entries.at[tuple(place)].set(high)


def block_scale(own_key, extent, cuts, low, high):
    factor_of, own = 1.0, jax.random.fold_in(own_key, 6)
    for dim, blocks in cuts:
        steps = jnp.exp(jax.random.uniform(jax.random.fold_in(own, dim), (blocks,), jnp.float32, low / len(cuts), high / len(cuts)))
        factor_of = factor_of * jnp.repeat(steps, extent[dim] // blocks).reshape([-1 if axis == dim else 1 for axis in range(len(extent))])
    return factor_of


def centred(rng, shape, width, most, pieces=(), kind=jnp.bfloat16):
    loudness = block_scale(rng, shape, pieces, -0.22, 0.18) if pieces else 1.0
    values = jax.random.normal(rng, shape, jnp.float32) * width * loudness
    return jnp.minimum(jnp.maximum(values, -most), most).astype(kind)


def setup_inputs(seed: int = 0) -> dict:
    arg_keys = jax.random.split(jax.random.key(seed), 14)
    return {
        "cameras": draw_cameras(jax.random.fold_in(arg_keys[13], 71), 0),
        "increment": draw_increment(jax.random.fold_in(arg_keys[13], 71), 0),
        "points": draw_points(jax.random.fold_in(arg_keys[13], 71), 0),
        "point_gradient": centred(arg_keys[3], (3, NPTS), 0.3, 1.8, ((1, 8),), jnp.float32),
        "point_inverse": draw_point_inverse(jax.random.fold_in(arg_keys[13], 71), 0),
        "cam_jacobian": centred(arg_keys[5], (18, NOBS), 0.5, 3.0, ((1, 32),)),
        "point_jacobian": centred(arg_keys[6], (6, NOBS), 0.5, 3.0, ((1, 32),)),
        "observed": draw_observed(jax.random.fold_in(arg_keys[13], 71), 0),
        "tile_block": plant(jax.random.randint(arg_keys[8], (NOBS // TILE,), 0, CAMS // CB), jax.random.fold_in(arg_keys[8], 1), 0, (CAMS // CB) - 1).astype(jnp.int32),
        "tile_points": plant(jax.random.randint(arg_keys[9], (NOBS // TILE,), 0, PTS_DEV // PB), jax.random.fold_in(arg_keys[9], 1), 0, (PTS_DEV // PB) - 1).astype(jnp.int32),
        "obs_camera": plant(jax.random.randint(arg_keys[10], (NOBS,), 0, CB), jax.random.fold_in(arg_keys[10], 1), 0, CB - 1).astype(jnp.int32),
        "obs_point": plant(jax.random.randint(arg_keys[11], (NOBS,), 0, PB), jax.random.fold_in(arg_keys[11], 1), 0, PB - 1).astype(jnp.int32),
        "accept": jax.random.randint(arg_keys[12], (), 0, 1073741824).astype(jnp.int32),
    }


def rotate_point(angles, coords):
    angle_size = jnp.sqrt(lax.optimization_barrier(jnp.sum(angles * angles, axis=0)))
    cosine = jnp.cos(angle_size)
    sine_ratio = jnp.sinc(angle_size / math.pi)
    cosine_ratio = 0.5 * jnp.square(jnp.sinc(angle_size / (2.0 * math.pi)))
    crossed = jnp.stack([angles[1] * coords[2] - angles[2] * coords[1], angles[2] * coords[0] - angles[0] * coords[2], angles[0] * coords[1] - angles[1] * coords[0]])
    inner_part = lax.optimization_barrier(jnp.sum(angles * coords, axis=0))
    return cosine * coords + sine_ratio * crossed + cosine_ratio * inner_part * angles

def project(camera, coords):
    placed = rotate_point(camera[0:3], coords) + camera[3:6]
    depth_clip = jnp.maximum(-placed[2], 1.0)
    planar = placed[0:2] / depth_clip
    radius = lax.optimization_barrier(jnp.sum(planar * planar, axis=0))
    factor = camera[6] * (1.0 + camera[7] * radius + camera[8] * radius * radius)
    return factor * planar

def couple(cam_rows, point_rows, cam_steps):
    cam_rows = cam_rows.astype(jnp.float32)
    point_rows = point_rows.astype(jnp.float32)
    first_row = lax.optimization_barrier(jnp.sum(cam_rows[0:9] * cam_steps, axis=0))
    second_row = lax.optimization_barrier(jnp.sum(cam_rows[9:18] * cam_steps, axis=0))
    return point_rows[0:3] * first_row + point_rows[3:6] * second_row

def solve_points(inverse, gradient, reduced):
    residue = gradient - reduced
    return jnp.stack([inverse[3 * target] * residue[0] + inverse[3 * target + 1] * residue[1] + inverse[3 * target + 2] * residue[2] for target in range(3)])

def reference(cameras, increment, points, point_gradient, point_inverse, cam_jacobian, point_jacobian, observed, tile_block, tile_points, obs_camera, obs_point, accept):
    trial_cameras = cameras + increment
    group_tiles = OBS_GROUP // TILE

    def segment_rows(values, owners):
        return jax.ops.segment_sum(values, owners, num_segments=PTS_DEV)

    def one_group(group_id):
        obs_start = (group_id * OBS_GROUP).astype(jnp.int32)
        tile_start = (group_id * group_tiles).astype(jnp.int32)
        chosen = lax.dynamic_slice_in_dim(tile_block, tile_start, group_tiles, 0)
        chosen_points = lax.dynamic_slice_in_dim(tile_points, tile_start, group_tiles, 0)
        cam_local = lax.dynamic_slice_in_dim(obs_camera, obs_start, OBS_GROUP, 0)
        cam_which = (jnp.repeat(chosen, TILE) * CB + cam_local).astype(jnp.int32)
        step_rows = jnp.take(increment, cam_which, axis=1)
        trial_rows = jnp.take(trial_cameras, cam_which, axis=1)
        coupling = couple(lax.dynamic_slice_in_dim(cam_jacobian, obs_start, OBS_GROUP, 1), lax.dynamic_slice_in_dim(point_jacobian, obs_start, OBS_GROUP, 1), step_rows)
        point_local = lax.dynamic_slice_in_dim(obs_point, obs_start, OBS_GROUP, 0)
        owners = (jnp.repeat(chosen_points, TILE) * PB + point_local).astype(jnp.int32)
        reduced = jax.vmap(segment_rows, in_axes=(0, None))(coupling, owners)
        point_start = (group_id * PTS_DEV).astype(jnp.int32)
        own_points = lax.dynamic_slice_in_dim(points, point_start, PTS_DEV, 1)
        point_step = solve_points(lax.dynamic_slice_in_dim(point_inverse, point_start, PTS_DEV, 1), lax.dynamic_slice_in_dim(point_gradient, point_start, PTS_DEV, 1), reduced)
        seen_points = jnp.take(own_points + point_step, owners, axis=1)
        residual = project(trial_rows, seen_points) - lax.dynamic_slice_in_dim(observed, obs_start, OBS_GROUP, 1)
        return (residual, point_step, jnp.sum(residual * residual))
    residuals, point_steps, partials = lax.map(one_group, jnp.arange(N_PTS, dtype=jnp.int32))
    residual = jnp.transpose(residuals, (1, 0, 2)).reshape(2, NOBS)
    point_step = jnp.transpose(point_steps, (1, 0, 2)).reshape(3, NPTS)
    trial_cost = jnp.sum(partials) / (2.0 * NOBS)
    accepted_flag = jnp.remainder(accept, 2).astype(jnp.float32)
    return (residual, trial_cost, points + accepted_flag * point_step, cameras + accepted_flag * increment)
```

```python
import functools
import math

import jax
import jax.numpy as jnp
from jax import lax
from jax.experimental import pallas as pl
from jax.experimental.pallas import tpu as pltpu
from jax.sharding import PartitionSpec as P

CB = 128
PB = 256
TILE = 256
UNIT = 8
HI = 8
LO = 32
PITCH = 24


def lanes(table, index):
    return jnp.take_along_axis(table, index, axis=1, mode="promise_in_bounds")


def reduce_kernel(
    units, tb_ref, tp_ref, tab_ref, cj_ref, pj_ref, cam_ref, pt_ref, out_ref, acc, s1, t1, v1
):
    step = pl.program_id(0)
    steps = pl.num_programs(0)

    @pl.when(step == 0)
    def _():
        acc[...] = jnp.zeros_like(acc)

    iota8 = lax.broadcasted_iota(jnp.int32, (8, 128), 0)

    def unit(u, carry):
        first_tile = step * (units * UNIT) + u * UNIT
        span = UNIT * TILE
        cols = pl.ds(pl.multiple_of(u * span, span), span)
        cj = cj_ref[:, cols].astype(jnp.float32)
        pj = pj_ref[:, cols].astype(jnp.float32)
        for c in range(2 * UNIT):
            piece = slice(c * 128, c * 128 + 128)
            row = ((c % 2) * UNIT + c // 2) * PITCH
            s1[row : row + 18, :] = cj[:, piece]
            s1[row + 18 : row + 24, :] = pj[:, piece]
        for s in range(UNIT):
            b = tb_ref[first_tile + s]
            t1[pl.ds(s, 8, stride=8), :] = tab_ref[b, 0:8, :]
            t1[64 + s : 65 + s, :] = tab_ref[b, 8:9, :]
        for half in range(2):
            def dense(r):
                return s1[pl.ds(half * UNIT * PITCH + r, UNIT, stride=PITCH), :]

            ids = cam_ref[pl.ds(u * 16 + half, UNIT, stride=2), :]
            first = second = None
            for m in range(9):
                g = lanes(t1[m * 8 : m * 8 + 8, :], ids)
                a, b2 = dense(m) * g, dense(9 + m) * g
                first = a if first is None else first + a
                second = b2 if second is None else second + b2
            for n in range(3):
                value = dense(18 + n) * first + dense(21 + n) * second
                big = value.astype(jnp.bfloat16).astype(jnp.float32)
                row = (half * 6 + n) * 8
                v1[row : row + 8, :] = big
                v1[row + 24 : row + 32, :] = value - big
        for s in range(UNIT):
            left, right = [], []
            for half in range(2):
                ids = pt_ref[pl.ds(u * 16 + 2 * s + half, 8, stride=0), :]
                inside = (ids >> 5) == iota8
                low = ids & 31
                left.append(
                    jnp.concatenate(
                        [
                            jnp.where(inside, v1[pl.ds((half * 6 + r) * 8 + s, 8, stride=0), :], 0.0)
                            for r in range(6)
                        ],
                        axis=0,
                    )
                )
                right.append(
                    jnp.concatenate(
                        [jnp.where(low == iota8 + 8 * j, 1.0, 0.0) for j in range(4)], axis=0
                    )
                )
            both = lax.dot_general(
                jnp.concatenate(left, axis=1).astype(jnp.bfloat16),
                jnp.concatenate(right, axis=1).astype(jnp.bfloat16),
                (((1,), (1,)), ((), ())),
                preferred_element_type=jnp.float32,
            )
            p = tp_ref[first_tile + s]
            acc[p, :, 0:LO] += both[0:24] + both[24:48]
        return carry

    lax.fori_loop(0, units, unit, 0)

    @pl.when(step == steps - 1)
    def _():
        lane = lax.broadcasted_iota(jnp.int32, (8, 128), 1)
        mine = (lane >> 5) == (iota8 & 3)

        def block(g, carry):
            for j in range(4):
                for n in range(3):
                    v = acc[g * 4 + j, n * 8 : n * 8 + 8, :]
                    v = v + pltpu.roll(v, 32, 1)
                    v = v + pltpu.roll(v, 64, 1)
                    v = jnp.where(mine, v, 0.0)
                    v = v + pltpu.roll(v, 1, 0)
                    v = v + pltpu.roll(v, 2, 0)
                    t1[j * 2 + n * 8 : j * 2 + n * 8 + 1, :] = v[3:4]
                    t1[j * 2 + n * 8 + 1 : j * 2 + n * 8 + 2, :] = v[7:8]
            for n in range(3):
                out_ref[n, pl.ds(pl.multiple_of(g * 8, 8), 8), :] = t1[n * 8 : n * 8 + 8, :]
            return carry

        lax.fori_loop(0, acc.shape[0] // 4, block, 0)


def project_kernel(
    units, tb_ref, tp_ref, tab_ref, pts_ref, obs_ref, cam_ref, pt_ref, res_ref, cost_ref, ptab, t1, t2
):
    step = pl.program_id(0)

    @pl.when(step == 0)
    def _():
        cost_ref[...] = jnp.zeros_like(cost_ref)
        quarter = pts_ref.shape[2]
        per = quarter // 16

        def fill(g, carry):
            src = g // per
            c = (g % per) * 16
            for n in range(3):
                for lh in range(2):
                    rows = pts_ref[src, n, pl.ds(c + lh, 8, stride=2), :]
                    ptab[pl.ds(g * 64 + n * 2 + lh, 8, stride=8), :] = rows
            return carry

        lax.fori_loop(0, pts_ref.shape[0] * per, fill, 0)

    def unit(u, total):
        first_tile = step * (units * UNIT) + u * UNIT
        for s in range(UNIT):
            b = tb_ref[first_tile + s]
            t1[pl.ds(s, 8, stride=8), :] = tab_ref[b, 0:8, :]
            t1[pl.ds(64 + s, 8, stride=8), :] = tab_ref[b, 8:16, :]
            p = tp_ref[first_tile + s]
            t2[pl.ds(s, 8, stride=8), :] = ptab[pl.ds(pl.multiple_of(p * 8, 8), 8), :]
        for half in range(2):
            ids = cam_ref[pl.ds(u * 16 + half, UNIT, stride=2), :]
            pid = pt_ref[pl.ds(u * 16 + half, UNIT, stride=2), :]
            low = pid & 127
            upper = pid >= 128
            x = [
                jnp.where(
                    upper,
                    lanes(t2[n * 16 + 8 : n * 16 + 16, :], low),
                    lanes(t2[n * 16 : n * 16 + 8, :], low),
                )
                for n in range(3)
            ]
            q = [lanes(t1[m * 8 : m * 8 + 8, :], ids) for m in range(15)]
            placed = [
                q[3 * n] * x[0] + q[3 * n + 1] * x[1] + q[3 * n + 2] * x[2] + q[9 + n]
                for n in range(3)
            ]
            depth = jnp.maximum(-placed[2], 1.0)
            px, py = placed[0] / depth, placed[1] / depth
            radius = px * px + py * py
            factor = q[12] * (1.0 + q[13] * radius + q[14] * radius * radius)
            for r, plane in ((0, px), (1, py)):
                where = pl.ds(u * 32 + 2 * half + r, UNIT, stride=4)
                res = factor * plane - obs_ref[where, :]
                res_ref[where, :] = res
                total = total + res * res
        return total

    total = lax.fori_loop(0, units, unit, jnp.zeros((8, 128), jnp.float32))
    cost_ref[...] += total


def camera_rows(cameras, increment):
    trial = cameras + increment
    w = trial[0:3]
    size = jnp.sqrt(jnp.sum(w * w, axis=0))
    cosine = jnp.cos(size)
    s1 = jnp.sinc(size / math.pi)
    s2 = 0.5 * jnp.square(jnp.sinc(size / (2.0 * math.pi)))
    rows = [
        cosine + s2 * w[0] * w[0],
        s2 * w[0] * w[1] - s1 * w[2],
        s2 * w[0] * w[2] + s1 * w[1],
        s2 * w[1] * w[0] + s1 * w[2],
        cosine + s2 * w[1] * w[1],
        s2 * w[1] * w[2] - s1 * w[0],
        s2 * w[2] * w[0] - s1 * w[1],
        s2 * w[2] * w[1] + s1 * w[0],
        cosine + s2 * w[2] * w[2],
    ]
    return jnp.concatenate([jnp.stack(rows), trial[3:9], increment], axis=0)


def spread(value, axis, size):
    parts = [value]
    for s in range(1, size):
        parts.append(lax.ppermute(value, axis, [(k, (k + s) % size) for k in range(size)]))
    return jnp.stack(parts)


def on_device(
    n_pts,
    n_cam,
    cameras,
    increment,
    points,
    point_gradient,
    point_inverse,
    cam_jacobian,
    point_jacobian,
    observed,
    tile_block,
    tile_points,
    obs_camera,
    obs_point,
    accept,
):
    both = ("pts", "cam")
    mine = camera_rows(cameras, increment)
    table = lax.all_to_all(
        jnp.broadcast_to(mine[None], (n_pts * n_cam,) + mine.shape), both, 0, 0
    )
    blocks = table.shape[0] * table.shape[2] // CB
    table = table.reshape(table.shape[0], 24, -1, CB).transpose(0, 2, 1, 3).reshape(blocks, 24, CB)
    rot_table = jnp.pad(table[:, 0:15], ((0, 0), (0, 1), (0, 0)))
    inc_table = jnp.pad(table[:, 15:24], ((0, 0), (0, 7), (0, 0)))

    tiles = tile_block.shape[0]
    count = obs_camera.shape[0]
    point_count = points.shape[1]
    point_blocks = point_count // PB
    ids_cam = obs_camera.reshape(-1, 128)
    ids_pt = obs_point.reshape(-1, 128)
    steps = math.gcd(tiles // UNIT, 16)
    units = tiles // (UNIT * steps)
    obs_step = count // steps

    reduced = pl.pallas_call(
        functools.partial(reduce_kernel, units),
        out_shape=jax.ShapeDtypeStruct((3, point_count // 128, 128), jnp.float32),
        grid_spec=pltpu.PrefetchScalarGridSpec(
            num_scalar_prefetch=2,
            grid=(steps,),
            in_specs=[
                pl.BlockSpec((blocks, 16, CB), lambda i, a, b: (0, 0, 0)),
                pl.BlockSpec((18, obs_step), lambda i, a, b: (0, i)),
                pl.BlockSpec((6, obs_step), lambda i, a, b: (0, i)),
                pl.BlockSpec((obs_step // 128, 128), lambda i, a, b: (i, 0)),
                pl.BlockSpec((obs_step // 128, 128), lambda i, a, b: (i, 0)),
            ],
            out_specs=pl.BlockSpec((3, point_count // 128, 128), lambda i, a, b: (0, 0, 0)),
            scratch_shapes=[
                pltpu.VMEM((point_blocks, 24, 128), jnp.float32),
                pltpu.VMEM((2 * UNIT * PITCH, 128), jnp.float32),
                pltpu.VMEM((72, 128), jnp.float32),
                pltpu.VMEM((96, 128), jnp.float32),
            ],
        ),
        compiler_params=pltpu.CompilerParams(dimension_semantics=("arbitrary",)),
        name="reduce_points",
    )(tile_block, tile_points, inc_table, cam_jacobian, point_jacobian, ids_cam, ids_pt)

    me = lax.axis_index("cam")
    rows = point_count // 128 // n_cam
    parts = reduced.reshape(3, n_cam, rows, 128)
    summed = lax.dynamic_index_in_dim(parts, me, 1, False)
    for s in range(1, n_cam):
        piece = lax.dynamic_index_in_dim(parts, lax.rem(me + s, n_cam), 1, False)
        summed = summed + lax.ppermute(piece, "cam", [(k, (k + s) % n_cam) for k in range(n_cam)])

    def own(array):
        part = lax.dynamic_slice_in_dim(array, me * (rows * 128), rows * 128, 1)
        return part.reshape(array.shape[0], rows, 128)

    residue = own(point_gradient) - summed
    inverse = own(point_inverse)
    point_step = jnp.stack(
        [
            inverse[3 * i] * residue[0]
            + inverse[3 * i + 1] * residue[1]
            + inverse[3 * i + 2] * residue[2]
            for i in range(3)
        ]
    )
    trial = spread(own(points) + point_step, "cam", n_cam)
    trial = jnp.take(trial, jnp.mod(me - jnp.arange(n_cam), n_cam), axis=0)

    obs_rows = observed.reshape(2, -1, 128).transpose(1, 0, 2).reshape(-1, 128)
    residual, partial = pl.pallas_call(
        functools.partial(project_kernel, units),
        out_shape=(
            jax.ShapeDtypeStruct(obs_rows.shape, jnp.float32),
            jax.ShapeDtypeStruct((8, 128), jnp.float32),
        ),
        grid_spec=pltpu.PrefetchScalarGridSpec(
            num_scalar_prefetch=2,
            grid=(steps,),
            in_specs=[
                pl.BlockSpec((blocks, 16, CB), lambda i, a, b: (0, 0, 0)),
                pl.BlockSpec((n_cam, 3, rows, 128), lambda i, a, b: (0, 0, 0, 0)),
                pl.BlockSpec((obs_step // 64, 128), lambda i, a, b: (i, 0)),
                pl.BlockSpec((obs_step // 128, 128), lambda i, a, b: (i, 0)),
                pl.BlockSpec((obs_step // 128, 128), lambda i, a, b: (i, 0)),
            ],
            out_specs=(
                pl.BlockSpec((obs_step // 64, 128), lambda i, a, b: (i, 0)),
                pl.BlockSpec((8, 128), lambda i, a, b: (0, 0)),
            ),
            scratch_shapes=[
                pltpu.VMEM((point_blocks * 8, 128), jnp.float32),
                pltpu.VMEM((128, 128), jnp.float32),
                pltpu.VMEM((64, 128), jnp.float32),
            ],
        ),
        compiler_params=pltpu.CompilerParams(dimension_semantics=("arbitrary",)),
        name="project_points",
    )(tile_block, tile_points, rot_table, trial, obs_rows, ids_cam, ids_pt)
    residual = residual.reshape(-1, 2, 128).transpose(1, 0, 2).reshape(2, -1)

    partial = jnp.sum(partial, axis=0, keepdims=True)
    spread_sums = lax.all_to_all(
        jnp.broadcast_to(partial, (n_pts * n_cam, 128)), both, 0, 0
    )
    trial_cost = jnp.sum(spread_sums) / (2.0 * count * n_pts * n_cam)
    flag = jnp.remainder(accept, 2).astype(jnp.float32)
    trial_natural = trial.transpose(1, 0, 2, 3).reshape(3, point_count)
    accepted_points = jnp.where(flag > 0.0, trial_natural, points)
    return residual, trial_cost, accepted_points, cameras + flag * increment


def solution(mesh):
    in_specs = (
        P(None, ("pts", "cam")),
        P(None, ("pts", "cam")),
        P(None, "pts"),
        P(None, "pts"),
        P(None, "pts"),
        P(None, ("pts", "cam")),
        P(None, ("pts", "cam")),
        P(None, ("pts", "cam")),
        P(("pts", "cam")),
        P(("pts", "cam")),
        P(("pts", "cam")),
        P(("pts", "cam")),
        P(),
    )
    out_specs = (P(None, ("pts", "cam")), P(), P(None, "pts"), P(None, ("pts", "cam")))
    body = functools.partial(on_device, mesh.shape["pts"], mesh.shape["cam"])
    return jax.shard_map(body, mesh=mesh, in_specs=in_specs, out_specs=out_specs, check_vma=False)
```

```python
import functools
import math

import jax
import jax.numpy as jnp
from jax import lax
from jax.experimental import pallas as pl
from jax.experimental.pallas import tpu as pltpu
from jax.sharding import PartitionSpec as P

CB = 128
PB = 256
TILE = 256
UNIT = 8
HI = 8
LO = 32
PITCH = 28
WAYS = 16
WAYS2 = 16
CHUNKS = 8
GATHER = 16
AHEAD = 2


def lanes(table, index):
    return jnp.take_along_axis(table, index, axis=1, mode="promise_in_bounds")


def arrivals(chunks, pairs, sems):
    def copies(c):
        out = []
        for k, (src, dst, axis) in enumerate(pairs):
            size = src.shape[axis] // chunks
            piece = pl.ds(pl.multiple_of(c * size, size), size)
            where = (slice(None), piece) if axis else (piece, slice(None))
            out.append(pltpu.make_async_copy(src.at[where], dst.at[where], sems.at[c, k]))
        return out

    def start(c):
        @pl.when(c < chunks)
        def _():
            for copy in copies(c):
                copy.start()

    def wait(c):
        for copy in copies(c):
            copy.wait()

    return start, wait


def reduce_kernel(
    n_cam, me_ref, tb_ref, tp_ref, tab_ref, cj_hbm, pj_hbm, cam_hbm, pt_hbm, *refs
):
    out_refs, refs = refs[:n_cam], refs[n_cam:]
    reduce_body(
        me_ref, tb_ref, tp_ref, tab_ref, cj_hbm, pj_hbm, cam_hbm, pt_hbm, out_refs, *refs
    )


def reduce_body(
    me_ref, tb_ref, tp_ref, tab_ref, cj_hbm, pj_hbm, cam_hbm, pt_hbm, out_refs,
    cj_ref, pj_ref, cam_ref, pt_ref, sems, fin, acc, *scratch
):
    s1s = scratch[:WAYS]
    t1s = scratch[WAYS : 2 * WAYS]
    v1s = scratch[2 * WAYS : 3 * WAYS]
    chunks = sems.shape[0]
    trips = cam_ref.shape[0] // (2 * UNIT * WAYS * chunks)
    start, wait = arrivals(
        chunks,
        ((cj_hbm, cj_ref, 1), (pj_hbm, pj_ref, 1), (cam_hbm, cam_ref, 0), (pt_hbm, pt_ref, 0)),
        sems,
    )
    for c in range(AHEAD):
        start(c)
    acc[...] = jnp.zeros_like(acc)

    iota8 = lax.broadcasted_iota(jnp.int32, (8, 128), 0)

    def couple(u, s1, t1, v1):
        first_tile = u * UNIT
        span = UNIT * TILE
        cols = pl.ds(pl.multiple_of(u * span, span), span)
        cj = cj_ref[:, cols].astype(jnp.float32)
        pj = pj_ref[:, cols].astype(jnp.float32)
        for c in range(2 * UNIT):
            piece = slice(c * 128, c * 128 + 128)
            row = ((c % 2) * UNIT + c // 2) * PITCH
            s1[row : row + 18, :] = cj[:, piece]
            s1[row + 18 : row + 24, :] = pj[:, piece]
        for s in range(UNIT):
            b = tb_ref[first_tile + s]
            t1[pl.ds(s, 8, stride=9), :] = tab_ref[b, 0:8, :]
            t1[72 + s : 73 + s, :] = tab_ref[b, 8:9, :]
        for half in range(2):

            def dense(r):
                return s1[pl.ds(half * UNIT * PITCH + r, UNIT, stride=PITCH), :]

            ids = cam_ref[pl.ds(u * 16 + half, UNIT, stride=2), :]
            first = second = None
            for m in range(9):
                g = lanes(t1[m * 9 : m * 9 + 8, :], ids)
                a, b2 = dense(m) * g, dense(9 + m) * g
                first = a if first is None else first + a
                second = b2 if second is None else second + b2
            for n in range(3):
                value = dense(18 + n) * first + dense(21 + n) * second
                big = value.astype(jnp.bfloat16).astype(jnp.float32)
                row = (half * 6 + n) * 8
                v1[row : row + 8, :] = big
                v1[row + 24 : row + 32, :] = value - big

    def products(u, v1):
        sums = []
        for s in range(UNIT):
            left, right = [], []
            for half in range(2):
                ids = pt_ref[pl.ds(u * 16 + 2 * s + half, 8, stride=0), :]
                inside = (ids >> 5) == iota8
                low = ids & 31
                left.append(
                    jnp.concatenate(
                        [
                            jnp.where(inside, v1[pl.ds((half * 6 + r) * 8 + s, 8, stride=0), :], 0.0)
                            for r in range(6)
                        ],
                        axis=0,
                    )
                )
                right.append(
                    jnp.concatenate(
                        [jnp.where(low == iota8 + 8 * j, 1.0, 0.0) for j in range(4)], axis=0
                    )
                )
            both = lax.dot_general(
                jnp.concatenate(left, axis=1).astype(jnp.bfloat16),
                jnp.concatenate(right, axis=1).astype(jnp.bfloat16),
                (((1,), (1,)), ((), ())),
                preferred_element_type=jnp.float32,
            )
            sums.append(both[0:24] + both[24:48])
        return sums

    def store(u, sums):
        for s in range(0, UNIT, 2):
            p0, p1 = tp_ref[u * UNIT + s], tp_ref[u * UNIT + s + 1]
            old0, old1 = acc[p0, :, 0:LO], acc[p1, :, 0:LO]
            acc[p0, :, 0:LO] = old0 + sums[s]
            acc[p1, :, 0:LO] = old1 + (sums[s + 1] + jnp.where(p0 == p1, sums[s], 0.0))

    def chunk(c, carry):
        start(c + AHEAD)
        wait(c)

        def trip(i, carry):
            first = (c * trips + i) * WAYS
            for w in range(WAYS):
                couple(first + w, s1s[w], t1s[w], v1s[w])
            for w in range(WAYS):
                store(first + w, products(first + w, v1s[w]))
            return carry

        return lax.fori_loop(0, trips, trip, carry)

    lax.fori_loop(0, chunks, chunk, 0)

    lane = lax.broadcasted_iota(jnp.int32, (8, 128), 1)
    mine = (lane >> 5) == (iota8 & 3)
    groups = out_refs[0].shape[1] // 8
    gather = math.gcd(groups, GATHER)

    for slot, out_ref in enumerate(out_refs):
        base = lax.rem(me_ref[0] + slot, len(out_refs)) * groups

        def part(i, carry, out_ref=out_ref, base=base):
            for g in range(gather):
                for j in range(4):
                    for n in range(3):
                        b = (base + i * gather + g) * 4 + j
                        v = acc[b, n * 8 : n * 8 + 8, :]
                        v = v + pltpu.roll(v, 32, 1)
                        v = v + pltpu.roll(v, 64, 1)
                        v = jnp.where(mine, v, 0.0)
                        v = v + pltpu.roll(v, 1, 0)
                        v = v + pltpu.roll(v, 2, 0)
                        row = g * 24 + n * 8 + j * 2
                        fin[row : row + 1, :] = v[3:4]
                        fin[row + 1 : row + 2, :] = v[7:8]
            for g in range(gather):
                rows = pl.ds(pl.multiple_of((i * gather + g) * 8, 8), 8)
                for n in range(3):
                    out_ref[n, rows, :] = fin[g * 24 + n * 8 : g * 24 + n * 8 + 8, :]
            return carry

        lax.fori_loop(0, groups // gather, part, 0)


def project_kernel(
    n_cam, me_ref, tb_ref, tp_ref, tab_ref, *refs
):
    project_body(me_ref, tb_ref, tp_ref, tab_ref, refs[:n_cam], *refs[n_cam:])


def project_body(
    me_ref, tb_ref, tp_ref, tab_ref, pts_refs, obs_hbm, cam_hbm, pt_hbm, res_hbm, cost_ref,
    obs_ref, cam_ref, pt_ref, res_ref, sems, out_sems, ptab, *scratch
):
    t1s, t2s = scratch[:WAYS2], scratch[WAYS2:]
    chunks = sems.shape[0]
    trips = cam_ref.shape[0] // (2 * UNIT * WAYS2 * chunks)
    start, wait = arrivals(
        chunks, ((obs_hbm, obs_ref, 0), (cam_hbm, cam_ref, 0), (pt_hbm, pt_ref, 0)), sems
    )
    for c in range(AHEAD):
        start(c)
    per = pts_refs[0].shape[1] // 16
    for slot, pts_ref in enumerate(pts_refs):
        base = lax.rem(me_ref[0] + len(pts_refs) - slot, len(pts_refs)) * per

        def fill(g, carry, pts_ref=pts_ref, base=base):
            for n in range(3):
                for lh in range(2):
                    rows = pts_ref[n, pl.ds(g * 16 + lh, 8, stride=2), :]
                    ptab[pl.ds((base + g) * 64 + n * 2 + lh, 8, stride=8), :] = rows
            return carry

        lax.fori_loop(0, per, fill, 0)

    def project(u, t1, t2, total):
        first_tile = u * UNIT
        for s in range(UNIT):
            b = tb_ref[first_tile + s]
            t1[pl.ds(s, 8, stride=9), :] = tab_ref[b, 0:8, :]
            t1[pl.ds(72 + s, 8, stride=9), :] = tab_ref[b, 8:16, :]
            p = tp_ref[first_tile + s]
            t2[pl.ds(s, 8, stride=9), :] = ptab[pl.ds(pl.multiple_of(p * 8, 8), 8), :]
        for half in range(2):
            ids = cam_ref[pl.ds(u * 16 + half, UNIT, stride=2), :]
            pid = pt_ref[pl.ds(u * 16 + half, UNIT, stride=2), :]
            low = pid & 127
            upper = pid >= 128
            x = [
                jnp.where(
                    upper,
                    lanes(t2[n * 18 + 9 : n * 18 + 17, :], low),
                    lanes(t2[n * 18 : n * 18 + 8, :], low),
                )
                for n in range(3)
            ]
            q = [lanes(t1[m * 9 : m * 9 + 8, :], ids) for m in range(15)]
            placed = [
                q[3 * n] * x[0] + q[3 * n + 1] * x[1] + q[3 * n + 2] * x[2] + q[9 + n]
                for n in range(3)
            ]
            depth = jnp.maximum(-placed[2], 1.0)
            px, py = placed[0] / depth, placed[1] / depth
            radius = px * px + py * py
            factor = q[12] * (1.0 + q[13] * radius + q[14] * radius * radius)
            for r, plane in ((0, px), (1, py)):
                where = pl.ds(u * 32 + 2 * half + r, UNIT, stride=4)
                res = factor * plane - obs_ref[where, :]
                res_ref[where, :] = res
                total = total + res * res
        return total

    def leave(c):
        size = res_ref.shape[0] // chunks
        piece = pl.ds(pl.multiple_of(c * size, size), size)
        return pltpu.make_async_copy(res_ref.at[piece, :], res_hbm.at[piece, :], out_sems.at[c])

    def chunk(c, total):
        start(c + AHEAD)
        wait(c)

        def trip(i, total):
            first = (c * trips + i) * WAYS2
            for w in range(WAYS2):
                total = project(first + w, t1s[w], t2s[w], total)
            return total

        total = lax.fori_loop(0, trips, trip, total)
        leave(c).start()
        return total

    cost_ref[...] = lax.fori_loop(0, chunks, chunk, jnp.zeros((8, 128), jnp.float32))

    def left(c, carry):
        leave(c).wait()
        return carry

    lax.fori_loop(0, chunks, left, 0)


SMEM = pl.BlockSpec(memory_space=pltpu.SMEM)
VMEM = pl.BlockSpec(memory_space=pltpu.VMEM)
HBM = pl.BlockSpec(memory_space=pl.ANY)


def run_reduce(me, n_cam, tile_block, tile_points, table, cam_jac, point_jac, ids_cam, ids_pt, points):
    chunks = math.gcd(tile_block.shape[0] // (UNIT * WAYS), CHUNKS)
    streamed = (cam_jac, point_jac, ids_cam, ids_pt)
    return pl.pallas_call(
        functools.partial(reduce_kernel, n_cam),
        out_shape=(jax.ShapeDtypeStruct((3, points // 128 // n_cam, 128), jnp.float32),) * n_cam,
        in_specs=[SMEM] * 3 + [VMEM] + [HBM] * 4,
        out_specs=(VMEM,) * n_cam,
        scratch_shapes=[pltpu.VMEM(a.shape, a.dtype) for a in streamed]
        + [pltpu.SemaphoreType.DMA((chunks, len(streamed)))]
        + [pltpu.VMEM((GATHER * 24, 128), jnp.float32)]
        + [pltpu.VMEM((points // PB, 24, 128), jnp.float32)]
        + [pltpu.VMEM((2 * UNIT * PITCH, 128), jnp.float32)] * WAYS
        + [pltpu.VMEM((80, 128), jnp.float32)] * WAYS
        + [pltpu.VMEM((96, 128), jnp.float32)] * WAYS,
        name="reduce_points",
    )(me, tile_block, tile_points, table, *streamed)


def run_project(me, tile_block, tile_points, table, trial, obs_rows, ids_cam, ids_pt):
    chunks = math.gcd(tile_block.shape[0] // (UNIT * WAYS2), CHUNKS)
    streamed = (obs_rows, ids_cam, ids_pt)
    n_cam = len(trial)
    points = n_cam * trial[0].shape[1]
    return pl.pallas_call(
        functools.partial(project_kernel, n_cam),
        out_shape=(
            jax.ShapeDtypeStruct(obs_rows.shape, jnp.float32),
            jax.ShapeDtypeStruct((8, 128), jnp.float32),
        ),
        in_specs=[SMEM] * 3 + [VMEM] * (1 + n_cam) + [HBM] * 3,
        out_specs=(HBM, VMEM),
        scratch_shapes=[pltpu.VMEM(a.shape, a.dtype) for a in streamed]
        + [pltpu.VMEM(obs_rows.shape, jnp.float32)]
        + [pltpu.SemaphoreType.DMA((chunks, len(streamed))), pltpu.SemaphoreType.DMA((chunks,))]
        + [pltpu.VMEM((points * 4, 128), jnp.float32)]
        + [pltpu.VMEM((144, 128), jnp.float32)] * WAYS2
        + [pltpu.VMEM((72, 128), jnp.float32)] * WAYS2,
        name="project_points",
    )(me, tile_block, tile_points, table, *trial, *streamed)


def rotation_rows(cameras, increment):
    trial = cameras + increment
    w = trial[:, 0:3]
    size = jnp.sqrt(jnp.sum(w * w, axis=1))
    cosine = jnp.cos(size)
    s1 = jnp.sinc(size / math.pi)
    s2 = 0.5 * jnp.square(jnp.sinc(size / (2.0 * math.pi)))
    w = [w[:, 0], w[:, 1], w[:, 2]]
    rows = [
        cosine + s2 * w[0] * w[0],
        s2 * w[0] * w[1] - s1 * w[2],
        s2 * w[0] * w[2] + s1 * w[1],
        s2 * w[1] * w[0] + s1 * w[2],
        cosine + s2 * w[1] * w[1],
        s2 * w[1] * w[2] - s1 * w[0],
        s2 * w[2] * w[0] - s1 * w[1],
        s2 * w[2] * w[1] + s1 * w[0],
        cosine + s2 * w[2] * w[2],
    ]
    rows += [trial[:, m] for m in range(3, 9)] + [cosine]
    return jnp.stack(rows, axis=1)


def spread(value, axis, size):
    parts = [value]
    for s in range(1, size):
        parts.append(lax.ppermute(value, axis, [(k, (k + s) % size) for k in range(size)]))
    return parts


def on_device(
    n_pts,
    n_cam,
    cameras,
    increment,
    points,
    point_gradient,
    point_inverse,
    cam_jacobian,
    point_jacobian,
    observed,
    tile_block,
    tile_points,
    obs_camera,
    obs_point,
    accept,
):
    both = ("pts", "cam")
    mine = jnp.concatenate([increment, cameras], axis=0)
    table = lax.all_to_all(
        jnp.broadcast_to(mine[None], (n_pts * n_cam,) + mine.shape), both, 0, 0
    )
    blocks = table.shape[0] * table.shape[2] // CB
    table = table.reshape(table.shape[0], 18, -1, CB).transpose(0, 2, 1, 3).reshape(blocks, 18, CB)
    rot_table = rotation_rows(table[:, 9:18], table[:, 0:9])

    count = obs_camera.shape[0]
    point_count = points.shape[1]
    ids_cam = obs_camera.reshape(-1, 128)
    ids_pt = obs_point.reshape(-1, 128)
    me = lax.axis_index("cam")
    me_word = me.reshape(1).astype(jnp.int32)
    parts = run_reduce(
        me_word, n_cam, tile_block, tile_points, table, cam_jacobian, point_jacobian, ids_cam, ids_pt, point_count
    )

    summed = parts[0]
    for s in range(1, n_cam):
        summed = summed + lax.ppermute(
            parts[s], "cam", [(k, (k + s) % n_cam) for k in range(n_cam)]
        )
    rows = point_count // 128 // n_cam

    def own(array):
        part = lax.dynamic_slice_in_dim(array, me * (rows * 128), rows * 128, 1)
        return part.reshape(array.shape[0], rows, 128)

    residue = own(point_gradient) - summed
    inverse = own(point_inverse)
    point_step = jnp.stack(
        [
            inverse[3 * i] * residue[0]
            + inverse[3 * i + 1] * residue[1]
            + inverse[3 * i + 2] * residue[2]
            for i in range(3)
        ]
    )
    trial = spread(own(points) + point_step, "cam", n_cam)

    obs_rows = observed.reshape(2, -1, 128).transpose(1, 0, 2).reshape(-1, 128)
    residual, partial = run_project(
        me_word, tile_block, tile_points, rot_table, trial, obs_rows, ids_cam, ids_pt
    )
    residual = residual.reshape(-1, 2, 128).transpose(1, 0, 2).reshape(2, -1)

    partial = jnp.sum(partial, axis=0, keepdims=True)
    spread_sums = lax.all_to_all(
        jnp.broadcast_to(partial, (n_pts * n_cam, 128)), both, 0, 0
    )
    trial_cost = jnp.sum(spread_sums) / (2.0 * count * n_pts * n_cam)
    flag = jnp.remainder(accept, 2).astype(jnp.float32)
    trial = jnp.take(jnp.stack(trial), jnp.mod(me - jnp.arange(n_cam), n_cam), axis=0)
    trial_natural = trial.transpose(1, 0, 2, 3).reshape(3, point_count)
    accepted_points = jnp.where(flag > 0.0, trial_natural, points)
    return residual, trial_cost, accepted_points, cameras + flag * increment


def solution(mesh):
    in_specs = (
        P(None, ("pts", "cam")),
        P(None, ("pts", "cam")),
        P(None, "pts"),
        P(None, "pts"),
        P(None, "pts"),
        P(None, ("pts", "cam")),
        P(None, ("pts", "cam")),
        P(None, ("pts", "cam")),
        P(("pts", "cam")),
        P(("pts", "cam")),
        P(("pts", "cam")),
        P(("pts", "cam")),
        P(),
    )
    out_specs = (P(None, ("pts", "cam")), P(), P(None, "pts"), P(None, ("pts", "cam")))
    body = functools.partial(on_device, mesh.shape["pts"], mesh.shape["cam"])
    return jax.shard_map(body, mesh=mesh, in_specs=in_specs, out_specs=out_specs, check_vma=False)
```

```python
import functools
import math

import jax
import jax.numpy as jnp
from jax import lax
from jax.experimental import pallas as pl
from jax.experimental.pallas import tpu as pltpu
from jax.sharding import PartitionSpec as P

CB = 128
PB = 256
TILE = 256
UNIT = 8
LOOKED = 10
HI = 8
LO = 32
PITCH = 28
WAYS = 16
WAYS2 = 16
WAYS3 = 8
WORK = 1 << 24
CHUNKS = 8
GATHER = 16
AHEAD = 2


def lanes(table, index):
    return jnp.take_along_axis(table, index, axis=1, mode="promise_in_bounds")


def arrivals(chunks, pairs, sems):
    def copies(c):
        out = []
        for k, (src, dst, axis) in enumerate(pairs):
            size = src.shape[axis] // chunks
            piece = pl.ds(pl.multiple_of(c * size, size), size)
            where = (slice(None), piece) if axis else (piece, slice(None))
            out.append(pltpu.make_async_copy(src.at[where], dst.at[where], sems.at[c, k]))
        return out

    def start(c):
        @pl.when(c < chunks)
        def _():
            for copy in copies(c):
                copy.start()

    def wait(c):
        for copy in copies(c):
            copy.wait()

    return start, wait


def reduce_kernel(
    n_cam, me_ref, tb_ref, tp_ref, tab_ref, cj_hbm, pj_hbm, cam_hbm, pt_hbm, *refs
):
    out_refs, refs = refs[:n_cam], refs[n_cam:]
    reduce_body(
        me_ref, tb_ref, tp_ref, tab_ref, cj_hbm, pj_hbm, cam_hbm, pt_hbm, out_refs, *refs
    )


def reduce_body(
    me_ref, tb_ref, tp_ref, tab_ref, cj_hbm, pj_hbm, cam_hbm, pt_hbm, out_refs,
    cj_ref, pj_ref, cam_ref, pt_ref, sems, fin, acc, *scratch
):
    s1s = scratch[:WAYS]
    t1s = scratch[WAYS : 2 * WAYS]
    v1s = scratch[2 * WAYS : 3 * WAYS]
    chunks = sems.shape[0]
    trips = cam_ref.shape[0] // (2 * UNIT * WAYS * chunks)
    start, wait = arrivals(
        chunks,
        ((cj_hbm, cj_ref, 1), (pj_hbm, pj_ref, 1), (cam_hbm, cam_ref, 0), (pt_hbm, pt_ref, 0)),
        sems,
    )
    for c in range(AHEAD):
        start(c)
    acc[...] = jnp.zeros_like(acc)

    iota8 = lax.broadcasted_iota(jnp.int32, (8, 128), 0)

    def couple(u, s1, t1, v1):
        first_tile = u * UNIT
        span = UNIT * TILE
        cols = pl.ds(pl.multiple_of(u * span, span), span)
        cj = cj_ref[:, cols].astype(jnp.float32)
        pj = pj_ref[:, cols].astype(jnp.float32)
        for c in range(2 * UNIT):
            piece = slice(c * 128, c * 128 + 128)
            row = ((c % 2) * UNIT + c // 2) * PITCH
            s1[row : row + 18, :] = cj[:, piece]
            s1[row + 18 : row + 24, :] = pj[:, piece]
        for s in range(UNIT):
            b = tb_ref[first_tile + s]
            t1[pl.ds(s, 8, stride=9), :] = tab_ref[b, 0:8, :]
            t1[72 + s : 73 + s, :] = tab_ref[b, 8:9, :]
        for half in range(2):

            def dense(r):
                return s1[pl.ds(half * UNIT * PITCH + r, UNIT, stride=PITCH), :]

            ids = cam_ref[pl.ds(u * 16 + half, UNIT, stride=2), :]
            first = second = None
            for m in range(9):
                g = lanes(t1[m * 9 : m * 9 + 8, :], ids)
                a, b2 = dense(m) * g, dense(9 + m) * g
                first = a if first is None else first + a
                second = b2 if second is None else second + b2
            for n in range(3):
                value = dense(18 + n) * first + dense(21 + n) * second
                big = value.astype(jnp.bfloat16).astype(jnp.float32)
                row = (half * 6 + n) * 8
                v1[row : row + 8, :] = big
                v1[row + 24 : row + 32, :] = value - big

    def products(u, v1):
        sums = []
        for s in range(UNIT):
            left, right = [], []
            for half in range(2):
                ids = pt_ref[pl.ds(u * 16 + 2 * s + half, 8, stride=0), :]
                inside = (ids >> 5) == iota8
                low = ids & 31
                left.append(
                    jnp.concatenate(
                        [
                            jnp.where(inside, v1[pl.ds((half * 6 + r) * 8 + s, 8, stride=0), :], 0.0)
                            for r in range(6)
                        ],
                        axis=0,
                    )
                )
                right.append(
                    jnp.concatenate(
                        [jnp.where(low == iota8 + 8 * j, 1.0, 0.0) for j in range(4)], axis=0
                    )
                )
            both = lax.dot_general(
                jnp.concatenate(left, axis=1),
                jnp.concatenate(right, axis=1),
                (((1,), (1,)), ((), ())),
                preferred_element_type=jnp.float32,
            )
            sums.append(both[0:24] + both[24:48])
        return sums

    def store(u, sums):
        for s in range(0, UNIT, 2):
            p0, p1 = tp_ref[u * UNIT + s], tp_ref[u * UNIT + s + 1]
            old0, old1 = acc[p0, :, 0:LO], acc[p1, :, 0:LO]
            acc[p0, :, 0:LO] = old0 + sums[s]
            acc[p1, :, 0:LO] = old1 + (sums[s + 1] + jnp.where(p0 == p1, sums[s], 0.0))

    def chunk(c, carry):
        start(c + AHEAD)
        wait(c)

        def trip(i, carry):
            first = (c * trips + i) * WAYS
            for w in range(WAYS):
                couple(first + w, s1s[w], t1s[w], v1s[w])
            for w in range(WAYS):
                store(first + w, products(first + w, v1s[w]))
            return carry

        return lax.fori_loop(0, trips, trip, carry)

    lax.fori_loop(0, chunks, chunk, 0)

    lane = lax.broadcasted_iota(jnp.int32, (8, 128), 1)
    mine = (lane >> 5) == (iota8 & 3)
    groups = out_refs[0].shape[1] // 8
    gather = math.gcd(groups, GATHER)

    for slot, out_ref in enumerate(out_refs):
        base = lax.rem(me_ref[0] + slot, len(out_refs)) * groups

        def part(i, carry, out_ref=out_ref, base=base):
            for g in range(gather):
                for j in range(4):
                    for n in range(3):
                        b = (base + i * gather + g) * 4 + j
                        v = acc[b, n * 8 : n * 8 + 8, :]
                        v = v + pltpu.roll(v, 32, 1)
                        v = v + pltpu.roll(v, 64, 1)
                        v = jnp.where(mine, v, 0.0)
                        v = v + pltpu.roll(v, 1, 0)
                        v = v + pltpu.roll(v, 2, 0)
                        row = g * 24 + n * 8 + j * 2
                        fin[row : row + 1, :] = v[3:4]
                        fin[row + 1 : row + 2, :] = v[7:8]
            for g in range(gather):
                rows = pl.ds(pl.multiple_of((i * gather + g) * 8, 8), 8)
                for n in range(3):
                    out_ref[n, rows, :] = fin[g * 24 + n * 8 : g * 24 + n * 8 + 8, :]
            return carry

        lax.fori_loop(0, groups // gather, part, 0)


def look_kernel(after_ref, tb_ref, tab_ref, cam_hbm, out_hbm, cam_ref, out_ref, sems, out_sems, *t1s):
    chunks = sems.shape[0]
    trips = cam_ref.shape[0] // (2 * UNIT * WAYS3 * chunks)
    start, wait = arrivals(chunks, ((cam_hbm, cam_ref, 0),), sems)
    for c in range(AHEAD):
        start(c)

    def look(u, t1):
        for s in range(UNIT):
            b = tb_ref[u * UNIT + s]
            t1[pl.ds(s, 8, stride=9), :] = tab_ref[b, 0:8, :]
            t1[pl.ds(72 + s, 8, stride=9), :] = tab_ref[b, 8:16, :]
        for half in range(2):
            ids = cam_ref[pl.ds(u * 16 + half, UNIT, stride=2), :]
            base = (u * 2 + half) * (LOOKED * 8)
            for m in range(LOOKED):
                out_ref[pl.ds(pl.multiple_of(base + m * 8, 8), 8), :] = lanes(
                    t1[m * 9 : m * 9 + 8, :], ids
                )

    def leave(c):
        size = out_ref.shape[0] // chunks
        piece = pl.ds(pl.multiple_of(c * size, size), size)
        return pltpu.make_async_copy(out_ref.at[piece, :], out_hbm.at[piece, :], out_sems.at[c])

    def chunk(c, carry):
        start(c + AHEAD)
        wait(c)

        def trip(i, carry):
            for w in range(WAYS3):
                look((c * trips + i) * WAYS3 + w, t1s[w])
            return carry

        lax.fori_loop(0, trips, trip, 0)
        leave(c).start()
        return carry

    lax.fori_loop(0, chunks, chunk, 0)

    def left(c, carry):
        leave(c).wait()
        return carry

    lax.fori_loop(0, chunks, left, 0)


def project_kernel(n_cam, me_ref, tp_ref, *refs):
    project_body(me_ref, tp_ref, refs[:n_cam], *refs[n_cam:])


def project_body(
    me_ref, tp_ref, pts_refs, val_hbm, obs_hbm, pt_hbm, res_hbm, cost_ref,
    val_ref, obs_ref, pt_ref, res_ref, sems, out_sems, ptab, *t2s
):
    chunks = sems.shape[0]
    trips = pt_ref.shape[0] // (2 * UNIT * WAYS2 * chunks)
    start, wait = arrivals(
        chunks, ((val_hbm, val_ref, 0), (obs_hbm, obs_ref, 0), (pt_hbm, pt_ref, 0)), sems
    )
    for c in range(AHEAD):
        start(c)
    per = pts_refs[0].shape[1] // 16
    for slot, pts_ref in enumerate(pts_refs):
        base = lax.rem(me_ref[0] + len(pts_refs) - slot, len(pts_refs)) * per

        def fill(g, carry, pts_ref=pts_ref, base=base):
            for n in range(3):
                for lh in range(2):
                    rows = pts_ref[n, pl.ds(g * 16 + lh, 8, stride=2), :]
                    ptab[pl.ds((base + g) * 64 + n * 2 + lh, 8, stride=8), :] = rows
            return carry

        lax.fori_loop(0, per, fill, 0)

    def project(u, t2, total):
        for s in range(UNIT):
            p = tp_ref[u * UNIT + s]
            t2[pl.ds(s, 8, stride=9), :] = ptab[pl.ds(pl.multiple_of(p * 8, 8), 8), :]
        for half in range(2):
            pid = pt_ref[pl.ds(u * 16 + half, UNIT, stride=2), :]
            low = pid & 127
            upper = pid >= 128
            x = [
                jnp.where(
                    upper,
                    lanes(t2[n * 18 + 9 : n * 18 + 17, :], low),
                    lanes(t2[n * 18 : n * 18 + 8, :], low),
                )
                for n in range(3)
            ]
            base = (u * 2 + half) * (LOOKED * 8)
            q = [
                val_ref[pl.ds(pl.multiple_of(base + m * 8, 8), 8), :] for m in range(LOOKED)
            ]

            def cross(a, b):
                return [
                    a[1] * b[2] - a[2] * b[1],
                    a[2] * b[0] - a[0] * b[2],
                    a[0] * b[1] - a[1] * b[0],
                ]

            turned = cross(q[0:3], x)
            again = cross(q[0:3], turned)
            placed = [x[n] + q[3] * turned[n] + again[n] + q[4 + n] for n in range(3)]
            depth = jnp.maximum(-placed[2], 1.0)
            px, py = placed[0] / depth, placed[1] / depth
            radius = px * px + py * py
            factor = q[7] * (1.0 + q[8] * radius + q[9] * radius * radius)
            for r, plane in ((0, px), (1, py)):
                where = pl.ds(u * 32 + 2 * half + r, UNIT, stride=4)
                res = factor * plane - obs_ref[where, :]
                res_ref[where, :] = res
                total = total + res * res
        return total

    def leave(c):
        size = res_ref.shape[0] // chunks
        piece = pl.ds(pl.multiple_of(c * size, size), size)
        return pltpu.make_async_copy(res_ref.at[piece, :], res_hbm.at[piece, :], out_sems.at[c])

    def chunk(c, total):
        start(c + AHEAD)
        wait(c)

        def trip(i, total):
            first = (c * trips + i) * WAYS2
            for w in range(WAYS2):
                total = project(first + w, t2s[w], total)
            return total

        total = lax.fori_loop(0, trips, trip, total)
        leave(c).start()
        return total

    total = lax.fori_loop(0, chunks, chunk, jnp.zeros((8, 128), jnp.float32))
    total = jnp.sum(total, axis=0, keepdims=True)
    cost_ref[...] = jnp.broadcast_to(total[None], cost_ref.shape)

    def left(c, carry):
        leave(c).wait()
        return carry

    lax.fori_loop(0, chunks, left, 0)


SMEM = pl.BlockSpec(memory_space=pltpu.SMEM)
VMEM = pl.BlockSpec(memory_space=pltpu.VMEM)
HBM = pl.BlockSpec(memory_space=pl.ANY)


def run_reduce(me, n_cam, tile_block, tile_points, table, cam_jac, point_jac, ids_cam, ids_pt, points):
    chunks = math.gcd(tile_block.shape[0] // (UNIT * WAYS), CHUNKS)
    streamed = (cam_jac, point_jac, ids_cam, ids_pt)
    return pl.pallas_call(
        functools.partial(reduce_kernel, n_cam),
        out_shape=(jax.ShapeDtypeStruct((3, points // 128 // n_cam, 128), jnp.float32),) * n_cam,
        in_specs=[SMEM] * 3 + [VMEM] + [HBM] * 4,
        out_specs=(VMEM,) * n_cam,
        scratch_shapes=[pltpu.VMEM(a.shape, a.dtype) for a in streamed]
        + [pltpu.SemaphoreType.DMA((chunks, len(streamed)))]
        + [pltpu.VMEM((GATHER * 24, 128), jnp.float32)]
        + [pltpu.VMEM((points // PB, 24, 128), jnp.float32)]
        + [pltpu.VMEM((2 * UNIT * PITCH, 128), jnp.float32)] * WAYS
        + [pltpu.VMEM((80, 128), jnp.float32)] * WAYS
        + [pltpu.VMEM((96, 128), jnp.float32)] * WAYS,
        name="reduce_points",
    )(me, tile_block, tile_points, table, *streamed)


def run_look(after, tile_block, table, ids_cam):
    chunks = math.gcd(tile_block.shape[0] // (UNIT * WAYS3), CHUNKS)
    rows = ids_cam.shape[0] * LOOKED
    return pl.pallas_call(
        look_kernel,
        out_shape=jax.ShapeDtypeStruct((rows, 128), jnp.float32),
        in_specs=[HBM, SMEM, VMEM, HBM],
        out_specs=HBM,
        scratch_shapes=[
            pltpu.VMEM(ids_cam.shape, ids_cam.dtype),
            pltpu.VMEM((rows, 128), jnp.float32),
            pltpu.SemaphoreType.DMA((chunks, 1)),
            pltpu.SemaphoreType.DMA((chunks,)),
        ]
        + [pltpu.VMEM((144, 128), jnp.float32)] * WAYS3,
        cost_estimate=pl.CostEstimate(flops=WORK, bytes_accessed=rows * 512, transcendentals=0),
        name="look_up_cameras",
    )(after, tile_block, table, ids_cam)


def run_project(me, senders, tile_points, trial, values, obs_rows, ids_pt):
    chunks = math.gcd(tile_points.shape[0] // (UNIT * WAYS2), CHUNKS)
    streamed = (values, obs_rows, ids_pt)
    n_cam = len(trial)
    points = n_cam * trial[0].shape[1]
    return pl.pallas_call(
        functools.partial(project_kernel, n_cam),
        out_shape=(
            jax.ShapeDtypeStruct(obs_rows.shape, jnp.float32),
            jax.ShapeDtypeStruct((senders, 1, 128), jnp.float32),
        ),
        in_specs=[SMEM] * 2 + [VMEM] * n_cam + [HBM] * 3,
        out_specs=(HBM, VMEM),
        scratch_shapes=[pltpu.VMEM(a.shape, a.dtype) for a in streamed]
        + [pltpu.VMEM(obs_rows.shape, jnp.float32)]
        + [pltpu.SemaphoreType.DMA((chunks, len(streamed))), pltpu.SemaphoreType.DMA((chunks,))]
        + [pltpu.VMEM((points * 4, 128), jnp.float32)]
        + [pltpu.VMEM((72, 128), jnp.float32)] * WAYS2,
        name="project_points",
    )(me, tile_points, *trial, *streamed)


def trial_rows(cameras, increment):
    trial = cameras + increment
    w = trial[:, 0:3]
    size = jnp.sqrt(jnp.sum(w * w, axis=1, keepdims=True))
    vector = (math.sqrt(0.5) * jnp.sinc(size / (2.0 * math.pi))) * w
    scalar = math.sqrt(2.0) * jnp.cos(0.5 * size)
    rows = jnp.concatenate([vector, scalar, trial[:, 3:9]], axis=1)
    return jnp.pad(rows, ((0, 0), (0, 16 - LOOKED), (0, 0)))


def spread(value, axis, size):
    parts = [value]
    for s in range(1, size):
        parts.append(lax.ppermute(value, axis, [(k, (k + s) % size) for k in range(size)]))
    return parts


def on_device(
    n_pts,
    n_cam,
    cameras,
    increment,
    points,
    point_gradient,
    point_inverse,
    cam_jacobian,
    point_jacobian,
    observed,
    tile_block,
    tile_points,
    obs_camera,
    obs_point,
    accept,
):
    both = ("pts", "cam")
    mine = jnp.concatenate([increment, cameras], axis=0)
    table = lax.all_to_all(
        jnp.broadcast_to(mine[None], (n_pts * n_cam,) + mine.shape), both, 0, 0
    )
    blocks = table.shape[0] * table.shape[2] // CB
    table = table.reshape(table.shape[0], 18, -1, CB).transpose(0, 2, 1, 3).reshape(blocks, 18, CB)
    looked_table = trial_rows(table[:, 9:18], table[:, 0:9])

    count = obs_camera.shape[0]
    point_count = points.shape[1]
    ids_cam = obs_camera.reshape(-1, 128)
    ids_pt = obs_point.reshape(-1, 128)
    me = lax.axis_index("cam")
    me_word = me.reshape(1).astype(jnp.int32)
    parts = run_reduce(
        me_word, n_cam, tile_block, tile_points, table, cam_jacobian, point_jacobian, ids_cam, ids_pt, point_count
    )

    summed = parts[0]
    for s in range(1, n_cam):
        summed = summed + lax.ppermute(
            parts[s], "cam", [(k, (k + s) % n_cam) for k in range(n_cam)]
        )
    values = run_look(parts[0], tile_block, looked_table, ids_cam)
    rows = point_count // 128 // n_cam

    def own(array):
        part = lax.dynamic_slice_in_dim(array, me * (rows * 128), rows * 128, 1)
        return part.reshape(array.shape[0], rows, 128)

    residue = own(point_gradient) - summed
    inverse = own(point_inverse)
    point_step = jnp.stack(
        [
            inverse[3 * i] * residue[0]
            + inverse[3 * i + 1] * residue[1]
            + inverse[3 * i + 2] * residue[2]
            for i in range(3)
        ]
    )
    trial = spread(own(points) + point_step, "cam", n_cam)

    obs_rows = observed.reshape(2, -1, 128).transpose(1, 0, 2).reshape(-1, 128)
    residual, partial = run_project(
        me_word, n_pts * n_cam, tile_points, trial, values, obs_rows, ids_pt
    )
    residual = residual.reshape(-1, 2, 128).transpose(1, 0, 2).reshape(2, -1)

    spread_sums = lax.all_to_all(partial, both, 0, 0)
    trial_cost = jnp.sum(spread_sums) / (2.0 * count * n_pts * n_cam)
    flag = jnp.remainder(accept, 2).astype(jnp.float32)
    trial = jnp.take(jnp.stack(trial), jnp.mod(me - jnp.arange(n_cam), n_cam), axis=0)
    trial_natural = trial.transpose(1, 0, 2, 3).reshape(3, point_count)
    accepted_points = jnp.where(flag > 0.0, trial_natural, points)
    return residual, trial_cost, accepted_points, cameras + flag * increment


def solution(mesh):
    in_specs = (
        P(None, ("pts", "cam")),
        P(None, ("pts", "cam")),
        P(None, "pts"),
        P(None, "pts"),
        P(None, "pts"),
        P(None, ("pts", "cam")),
        P(None, ("pts", "cam")),
        P(None, ("pts", "cam")),
        P(("pts", "cam")),
        P(("pts", "cam")),
        P(("pts", "cam")),
        P(("pts", "cam")),
        P(),
    )
    out_specs = (P(None, ("pts", "cam")), P(), P(None, "pts"), P(None, ("pts", "cam")))
    body = functools.partial(on_device, mesh.shape["pts"], mesh.shape["cam"])
    return jax.shard_map(body, mesh=mesh, in_specs=in_specs, out_specs=out_specs, check_vma=False)
```

```python
import functools
import math

import jax
import jax.numpy as jnp
from jax import lax
from jax.experimental import pallas as pl
from jax.experimental.pallas import tpu as pltpu
from jax.sharding import PartitionSpec as P

CB = 128
PB = 256
TILE = 256
UNIT = 8
LOOKED = 10
HI = 8
LO = 32
PITCH = 28
WAYS = 16
WAYS2 = 16
WAYS3 = 8
WORK = 1 << 24
CHUNKS = 8
GATHER = 16
AHEAD = 2


def lanes(table, index):
    return jnp.take_along_axis(table, index, axis=1, mode="promise_in_bounds")


def arrivals(chunks, pairs, sems):
    def copies(c):
        out = []
        for k, (src, dst, axis) in enumerate(pairs):
            size = src.shape[axis] // chunks
            piece = pl.ds(pl.multiple_of(c * size, size), size)
            where = (slice(None), piece) if axis else (piece, slice(None))
            out.append(pltpu.make_async_copy(src.at[where], dst.at[where], sems.at[c, k]))
        return out

    def start(c):
        @pl.when(c < chunks)
        def _():
            for copy in copies(c):
                copy.start()

    def wait(c):
        for copy in copies(c):
            copy.wait()

    return start, wait


def reduce_kernel(
    n_cam, me_ref, tb_ref, tp_ref, tab_ref, cj_hbm, pj_hbm, cam_ref, pt_ref, *refs
):
    out_refs, refs = refs[:n_cam], refs[n_cam:]
    reduce_body(
        me_ref, tb_ref, tp_ref, tab_ref, cj_hbm, pj_hbm, cam_ref, pt_ref, out_refs, *refs
    )


def reduce_body(
    me_ref, tb_ref, tp_ref, tab_ref, cj_hbm, pj_hbm, cam_ref, pt_ref, out_refs,
    cj_ref, pj_ref, sems, fin, acc, *scratch
):
    s1s = scratch[:WAYS]
    t1s = scratch[WAYS : 2 * WAYS]
    v1s = scratch[2 * WAYS : 3 * WAYS]
    chunks = sems.shape[0]
    trips = cam_ref.shape[0] // (2 * UNIT * WAYS * chunks)
    start, wait = arrivals(chunks, ((cj_hbm, cj_ref, 1), (pj_hbm, pj_ref, 1)), sems)
    for c in range(AHEAD):
        start(c)
    acc[...] = jnp.zeros_like(acc)

    iota8 = lax.broadcasted_iota(jnp.int32, (8, 128), 0)

    def couple(u, s1, t1, v1):
        first_tile = u * UNIT
        span = UNIT * TILE
        cols = pl.ds(pl.multiple_of(u * span, span), span)
        cj = cj_ref[:, cols].astype(jnp.float32)
        pj = pj_ref[:, cols].astype(jnp.float32)
        for c in range(2 * UNIT):
            piece = slice(c * 128, c * 128 + 128)
            row = ((c % 2) * UNIT + c // 2) * PITCH
            s1[row : row + 18, :] = cj[:, piece]
            s1[row + 18 : row + 24, :] = pj[:, piece]
        for s in range(UNIT):
            b = tb_ref[first_tile + s]
            t1[pl.ds(s, 8, stride=9), :] = tab_ref[b, 0:8, :]
            t1[72 + s : 73 + s, :] = tab_ref[b, 8:9, :]
        for half in range(2):

            def dense(r):
                return s1[pl.ds(half * UNIT * PITCH + r, UNIT, stride=PITCH), :]

            ids = cam_ref[pl.ds(u * 16 + half, UNIT, stride=2), :]
            first = second = None
            for m in range(9):
                g = lanes(t1[m * 9 : m * 9 + 8, :], ids)
                a, b2 = dense(m) * g, dense(9 + m) * g
                first = a if first is None else first + a
                second = b2 if second is None else second + b2
            for n in range(3):
                value = dense(18 + n) * first + dense(21 + n) * second
                big = value.astype(jnp.bfloat16).astype(jnp.float32)
                row = (half * 6 + n) * 8
                v1[row : row + 8, :] = big
                v1[row + 24 : row + 32, :] = value - big

    def products(u, v1):
        sums = []
        for s in range(UNIT):
            left, right = [], []
            for half in range(2):
                ids = pt_ref[pl.ds(u * 16 + 2 * s + half, 8, stride=0), :]
                inside = (ids >> 5) == iota8
                low = ids & 31
                left.append(
                    jnp.concatenate(
                        [
                            jnp.where(inside, v1[pl.ds((half * 6 + r) * 8 + s, 8, stride=0), :], 0.0)
                            for r in range(6)
                        ],
                        axis=0,
                    )
                )
                right.append(
                    jnp.concatenate(
                        [jnp.where(low == iota8 + 8 * j, 1.0, 0.0) for j in range(4)], axis=0
                    )
                )
            both = lax.dot_general(
                jnp.concatenate(left, axis=1),
                jnp.concatenate(right, axis=1),
                (((1,), (1,)), ((), ())),
                preferred_element_type=jnp.float32,
            )
            sums.append(both[0:24] + both[24:48])
        return sums

    def store(u, sums):
        for s in range(0, UNIT, 2):
            p0, p1 = tp_ref[u * UNIT + s], tp_ref[u * UNIT + s + 1]
            old0, old1 = acc[p0, :, 0:LO], acc[p1, :, 0:LO]
            acc[p0, :, 0:LO] = old0 + sums[s]
            acc[p1, :, 0:LO] = old1 + (sums[s + 1] + jnp.where(p0 == p1, sums[s], 0.0))

    def chunk(c, carry):
        start(c + AHEAD)
        wait(c)

        def trip(i, carry):
            first = (c * trips + i) * WAYS
            for w in range(WAYS):
                couple(first + w, s1s[w], t1s[w], v1s[w])
            for w in range(WAYS):
                store(first + w, products(first + w, v1s[w]))
            return carry

        return lax.fori_loop(0, trips, trip, carry)

    lax.fori_loop(0, chunks, chunk, 0)

    lane = lax.broadcasted_iota(jnp.int32, (8, 128), 1)
    mine = (lane >> 5) == (iota8 & 3)
    groups = out_refs[0].shape[1] // 8
    gather = math.gcd(groups, GATHER)

    for slot, out_ref in enumerate(out_refs):
        base = lax.rem(me_ref[0] + slot, len(out_refs)) * groups

        def part(i, carry, out_ref=out_ref, base=base):
            for g in range(gather):
                for j in range(4):
                    for n in range(3):
                        b = (base + i * gather + g) * 4 + j
                        v = acc[b, n * 8 : n * 8 + 8, :]
                        v = v + pltpu.roll(v, 32, 1)
                        v = v + pltpu.roll(v, 64, 1)
                        v = jnp.where(mine, v, 0.0)
                        v = v + pltpu.roll(v, 1, 0)
                        v = v + pltpu.roll(v, 2, 0)
                        row = g * 24 + n * 8 + j * 2
                        fin[row : row + 1, :] = v[3:4]
                        fin[row + 1 : row + 2, :] = v[7:8]
            for g in range(gather):
                rows = pl.ds(pl.multiple_of((i * gather + g) * 8, 8), 8)
                for n in range(3):
                    out_ref[n, rows, :] = fin[g * 24 + n * 8 : g * 24 + n * 8 + 8, :]
            return carry

        lax.fori_loop(0, groups // gather, part, 0)


def look_kernel(after_ref, tb_ref, tab_ref, cam_ref, out_ref, *t1s):
    def look(u, t1):
        for s in range(UNIT):
            b = tb_ref[u * UNIT + s]
            t1[pl.ds(s, 8, stride=9), :] = tab_ref[b, 0:8, :]
            t1[pl.ds(72 + s, 8, stride=9), :] = tab_ref[b, 8:16, :]
        for half in range(2):
            ids = cam_ref[pl.ds(u * 16 + half, UNIT, stride=2), :]
            base = (u * 2 + half) * (LOOKED * 8)
            for m in range(LOOKED):
                out_ref[pl.ds(pl.multiple_of(base + m * 8, 8), 8), :] = lanes(
                    t1[m * 9 : m * 9 + 8, :], ids
                )

    def trip(i, carry):
        for w in range(WAYS3):
            look(i * WAYS3 + w, t1s[w])
        return carry

    lax.fori_loop(0, cam_ref.shape[0] // (2 * UNIT * WAYS3), trip, 0)


def project_kernel(n_cam, me_ref, tp_ref, *refs):
    project_body(me_ref, tp_ref, refs[:n_cam], *refs[n_cam:])


def project_body(
    me_ref, tp_ref, pts_refs, val_ref, obs_ref, pt_ref, res_hbm, cost_ref,
    res_ref, out_sems, ptab, *t2s
):
    chunks = out_sems.shape[0]
    trips = pt_ref.shape[0] // (2 * UNIT * WAYS2 * chunks)
    per = pts_refs[0].shape[1] // 16
    for slot, pts_ref in enumerate(pts_refs):
        base = lax.rem(me_ref[0] + len(pts_refs) - slot, len(pts_refs)) * per

        def fill(g, carry, pts_ref=pts_ref, base=base):
            for n in range(3):
                for lh in range(2):
                    rows = pts_ref[n, pl.ds(g * 16 + lh, 8, stride=2), :]
                    ptab[pl.ds((base + g) * 64 + n * 2 + lh, 8, stride=8), :] = rows
            return carry

        lax.fori_loop(0, per, fill, 0)

    def project(u, t2, total):
        for s in range(UNIT):
            p = tp_ref[u * UNIT + s]
            t2[pl.ds(s, 8, stride=9), :] = ptab[pl.ds(pl.multiple_of(p * 8, 8), 8), :]
        for half in range(2):
            pid = pt_ref[pl.ds(u * 16 + half, UNIT, stride=2), :]
            low = pid & 127
            upper = pid >= 128
            x = [
                jnp.where(
                    upper,
                    lanes(t2[n * 18 + 9 : n * 18 + 17, :], low),
                    lanes(t2[n * 18 : n * 18 + 8, :], low),
                )
                for n in range(3)
            ]
            base = (u * 2 + half) * (LOOKED * 8)
            q = [
                val_ref[pl.ds(pl.multiple_of(base + m * 8, 8), 8), :] for m in range(LOOKED)
            ]

            def cross(a, b):
                return [
                    a[1] * b[2] - a[2] * b[1],
                    a[2] * b[0] - a[0] * b[2],
                    a[0] * b[1] - a[1] * b[0],
                ]

            turned = cross(q[0:3], x)
            again = cross(q[0:3], turned)
            placed = [x[n] + q[3] * turned[n] + again[n] + q[4 + n] for n in range(3)]
            depth = jnp.maximum(-placed[2], 1.0)
            px, py = placed[0] / depth, placed[1] / depth
            radius = px * px + py * py
            factor = q[7] * (1.0 + q[8] * radius + q[9] * radius * radius)
            for r, plane in ((0, px), (1, py)):
                where = pl.ds(u * 32 + 2 * half + r, UNIT, stride=4)
                res = factor * plane - obs_ref[where, :]
                res_ref[where, :] = res
                total = total + res * res
        return total

    def leave(c):
        size = res_ref.shape[0] // chunks
        piece = pl.ds(pl.multiple_of(c * size, size), size)
        return pltpu.make_async_copy(res_ref.at[piece, :], res_hbm.at[piece, :], out_sems.at[c])

    def chunk(c, total):
        def trip(i, total):
            first = (c * trips + i) * WAYS2
            for w in range(WAYS2):
                total = project(first + w, t2s[w], total)
            return total

        total = lax.fori_loop(0, trips, trip, total)
        leave(c).start()
        return total

    total = lax.fori_loop(0, chunks, chunk, jnp.zeros((8, 128), jnp.float32))
    total = jnp.sum(total, axis=0, keepdims=True)
    cost_ref[...] = jnp.broadcast_to(total[None], cost_ref.shape)

    def left(c, carry):
        leave(c).wait()
        return carry

    lax.fori_loop(0, chunks, left, 0)


SMEM = pl.BlockSpec(memory_space=pltpu.SMEM)
VMEM = pl.BlockSpec(memory_space=pltpu.VMEM)
HBM = pl.BlockSpec(memory_space=pltpu.HBM)
ANY = pl.BlockSpec(memory_space=pl.ANY)


def offer_kernel(increment_ref, cameras_ref, out_ref):
    mine = jnp.concatenate([increment_ref[...], cameras_ref[...]], axis=0)
    out_ref[...] = jnp.broadcast_to(mine[None], out_ref.shape)


def run_offer(increment, cameras, receivers):
    rows = increment.shape[0] + cameras.shape[0]
    return pl.pallas_call(
        offer_kernel,
        out_shape=jax.ShapeDtypeStruct((receivers, rows, increment.shape[1]), jnp.float32),
        name="offer_cameras",
    )(increment, cameras)


def run_reduce(me, n_cam, tile_block, tile_points, table, cam_jac, point_jac, ids_cam, ids_pt, points):
    chunks = math.gcd(tile_block.shape[0] // (UNIT * WAYS), CHUNKS)
    streamed = (cam_jac, point_jac)
    return pl.pallas_call(
        functools.partial(reduce_kernel, n_cam),
        out_shape=(jax.ShapeDtypeStruct((3, points // 128 // n_cam, 128), jnp.float32),) * n_cam,
        in_specs=[SMEM] * 3 + [VMEM] + [HBM] * 2 + [VMEM] * 2,
        out_specs=(VMEM,) * n_cam,
        scratch_shapes=[pltpu.VMEM(a.shape, a.dtype) for a in streamed]
        + [pltpu.SemaphoreType.DMA((chunks, len(streamed)))]
        + [pltpu.VMEM((GATHER * 24, 128), jnp.float32)]
        + [pltpu.VMEM((points // PB, 24, 128), jnp.float32)]
        + [pltpu.VMEM((2 * UNIT * PITCH, 128), jnp.float32)] * WAYS
        + [pltpu.VMEM((80, 128), jnp.float32)] * WAYS
        + [pltpu.VMEM((96, 128), jnp.float32)] * WAYS,
        compiler_params=pltpu.CompilerParams(vmem_limit_bytes=58 << 20),
        name="reduce_points",
    )(me, tile_block, tile_points, table, *streamed, ids_cam, ids_pt)


def run_look(after, tile_block, table, ids_cam):
    rows = ids_cam.shape[0] * LOOKED
    return pl.pallas_call(
        look_kernel,
        out_shape=jax.ShapeDtypeStruct((rows, 128), jnp.float32),
        in_specs=[ANY, SMEM, VMEM, VMEM],
        out_specs=VMEM,
        scratch_shapes=[pltpu.VMEM((144, 128), jnp.float32)] * WAYS3,
        cost_estimate=pl.CostEstimate(flops=WORK, bytes_accessed=rows * 512, transcendentals=0),
        compiler_params=pltpu.CompilerParams(vmem_limit_bytes=24 << 20),
        name="look_up_cameras",
    )(after, tile_block, table, ids_cam)


def run_project(me, senders, tile_points, trial, values, obs_rows, ids_pt):
    chunks = math.gcd(tile_points.shape[0] // (UNIT * WAYS2), CHUNKS)
    n_cam = len(trial)
    points = n_cam * trial[0].shape[1]
    return pl.pallas_call(
        functools.partial(project_kernel, n_cam),
        out_shape=(
            jax.ShapeDtypeStruct(obs_rows.shape, jnp.float32),
            jax.ShapeDtypeStruct((senders, 1, 128), jnp.float32),
        ),
        in_specs=[SMEM] * 2 + [VMEM] * (n_cam + 3),
        out_specs=(HBM, VMEM),
        scratch_shapes=[pltpu.VMEM(obs_rows.shape, jnp.float32), pltpu.SemaphoreType.DMA((chunks,))]
        + [pltpu.VMEM((points * 4, 128), jnp.float32)]
        + [pltpu.VMEM((72, 128), jnp.float32)] * WAYS2,
        compiler_params=pltpu.CompilerParams(vmem_limit_bytes=28 << 20),
        name="project_points",
    )(me, tile_points, *trial, values, obs_rows, ids_pt)


def trial_rows(cameras, increment):
    trial = cameras + increment
    w = trial[:, 0:3]
    size = jnp.sqrt(jnp.sum(w * w, axis=1, keepdims=True))
    vector = (math.sqrt(0.5) * jnp.sinc(size / (2.0 * math.pi))) * w
    scalar = math.sqrt(2.0) * jnp.cos(0.5 * size)
    rows = jnp.concatenate([vector, scalar, trial[:, 3:9]], axis=1)
    return jnp.pad(rows, ((0, 0), (0, 16 - LOOKED), (0, 0)))


def spread(value, axis, size):
    parts = [value]
    for s in range(1, size):
        parts.append(lax.ppermute(value, axis, [(k, (k + s) % size) for k in range(size)]))
    return parts


def on_device(
    n_pts,
    n_cam,
    cameras,
    increment,
    points,
    point_gradient,
    point_inverse,
    cam_jacobian,
    point_jacobian,
    observed,
    tile_block,
    tile_points,
    obs_camera,
    obs_point,
    accept,
):
    both = ("pts", "cam")
    table = lax.all_to_all(run_offer(increment, cameras, n_pts * n_cam), both, 0, 0)
    blocks = table.shape[0] * table.shape[2] // CB
    table = table.reshape(table.shape[0], 18, -1, CB).transpose(0, 2, 1, 3).reshape(blocks, 18, CB)
    looked_table = trial_rows(table[:, 9:18], table[:, 0:9])

    count = obs_camera.shape[0]
    point_count = points.shape[1]
    ids_cam = obs_camera.reshape(-1, 128)
    ids_pt = obs_point.reshape(-1, 128)
    me = lax.axis_index("cam")
    me_word = me.reshape(1).astype(jnp.int32)
    parts = run_reduce(
        me_word, n_cam, tile_block, tile_points, table, cam_jacobian, point_jacobian, ids_cam, ids_pt, point_count
    )

    summed = parts[0]
    for s in range(1, n_cam):
        summed = summed + lax.ppermute(
            parts[s], "cam", [(k, (k + s) % n_cam) for k in range(n_cam)]
        )
    values = run_look(parts[0], tile_block, looked_table, ids_cam)
    rows = point_count // 128 // n_cam

    def own(array):
        part = lax.dynamic_slice_in_dim(array, me * (rows * 128), rows * 128, 1)
        return part.reshape(array.shape[0], rows, 128)

    residue = own(point_gradient) - summed
    inverse = own(point_inverse)
    point_step = jnp.stack(
        [
            inverse[3 * i] * residue[0]
            + inverse[3 * i + 1] * residue[1]
            + inverse[3 * i + 2] * residue[2]
            for i in range(3)
        ]
    )
    trial = spread(own(points) + point_step, "cam", n_cam)

    obs_rows = observed.reshape(2, -1, 128).transpose(1, 0, 2).reshape(-1, 128)
    residual, partial = run_project(
        me_word, n_pts * n_cam, tile_points, trial, values, obs_rows, ids_pt
    )
    residual = residual.reshape(-1, 2, 128).transpose(1, 0, 2).reshape(2, -1)

    spread_sums = lax.all_to_all(partial, both, 0, 0)
    trial_cost = jnp.sum(spread_sums) / (2.0 * count * n_pts * n_cam)
    flag = jnp.remainder(accept, 2).astype(jnp.float32)
    trial = jnp.take(jnp.stack(trial), jnp.mod(me - jnp.arange(n_cam), n_cam), axis=0)
    trial_natural = trial.transpose(1, 0, 2, 3).reshape(3, point_count)
    accepted_points = jnp.where(flag > 0.0, trial_natural, points)
    return residual, trial_cost, accepted_points, cameras + flag * increment


def solution(mesh):
    in_specs = (
        P(None, ("pts", "cam")),
        P(None, ("pts", "cam")),
        P(None, "pts"),
        P(None, "pts"),
        P(None, "pts"),
        P(None, ("pts", "cam")),
        P(None, ("pts", "cam")),
        P(None, ("pts", "cam")),
        P(("pts", "cam")),
        P(("pts", "cam")),
        P(("pts", "cam")),
        P(("pts", "cam")),
        P(),
    )
    out_specs = (P(None, ("pts", "cam")), P(), P(None, "pts"), P(None, ("pts", "cam")))
    body = functools.partial(on_device, mesh.shape["pts"], mesh.shape["cam"])
    return jax.shard_map(body, mesh=mesh, in_specs=in_specs, out_specs=out_specs, check_vma=False)
```
